16 devices in a mesh: dp: 2 (over y, z), tp: 8 (over x, core).
Axes of the slice: x: 4, y: 2, z: 1, core: 2. Of those that a mesh axis runs over, the one named last changes fastest.
The devices are a block of a 4x4x8 slice.
Arguments:
- x: bfloat16 [8, 2048, 5120], P('dp'), parts along dimension 0
- gamma: float32 [5120], replicated
- beta: float32 [5120], replicated
- wqkv: bfloat16 [5120, 15360], P(None, 'tp')
- wo: bfloat16 [40, 128, 5120], P('tp')
- w1: bfloat16 [5120, 20480], P(None, 'tp')
- w2: bfloat16 [20480, 5120], P('tp')
Outputs:
- output: bfloat16 [8, 2048, 5120], P('dp'), parts along dimension 0
There are 2 independent parts. The reference program is written for one: setup_inputs(seed, part) draws one part's arguments, and reference() takes and returns one part's arrays. A program takes and returns all parts, laid end to end along the dimension named above; an argument that names none is the same for every part.
All inputs are finite; a program needn't handle non-finite values.
Results may differ from the reference program's by a relative error of at most 0.0104394.
Values are sent between devices in bfloat16 or wider.
A program may use at most 768 MiB of HBM per device.

```python
import jax
import jax.numpy as jnp
from jax import lax

B = 4
S = 2048
D = 5120
HEADS = 40
KV = 40
HEAD = 128
FF = 20480


def setup_inputs(seed: int = 0, part: int = 0) -> dict:
    key = jax.random.key(seed)
    kx = jax.random.fold_in(jax.random.fold_in(key, 1), part)
    ks = jax.random.split(jax.random.fold_in(key, 2), 6)
    x = jax.random.normal(kx, (B, S, D), jnp.float32).astype(jnp.bfloat16)
    gamma = 1.0 + 0.3 * jax.random.normal(ks[0], (D,), jnp.float32)
    beta = 0.2 * jax.random.normal(ks[1], (D,), jnp.float32)
    wqkv = jax.random.normal(ks[2], (D, (HEADS + 2 * KV) * HEAD), jnp.float32) * D ** -0.5
    wo = jax.random.normal(ks[3], (HEADS, HEAD, D), jnp.float32) * ((HEADS * HEAD) ** -0.5 * 0.5 * S ** 0.25)
    w1 = jax.random.normal(ks[4], (D, FF), jnp.float32) * D ** -0.5
    w2 = jax.random.normal(ks[5], (FF, D), jnp.float32) * (0.7 * FF ** -0.5)
    return {'x': x, 'gamma': gamma, 'beta': beta,
            'wqkv': wqkv.astype(jnp.bfloat16), 'wo': wo.astype(jnp.bfloat16),
            'w1': w1.astype(jnp.bfloat16), 'w2': w2.astype(jnp.bfloat16)}


def layer_norm(x, gamma, beta):
    xf = x.astype(jnp.float32)
    mu = jnp.mean(xf, axis=-1, keepdims=True)
    var = jnp.mean(jnp.square(xf - mu), axis=-1, keepdims=True)
    return ((xf - mu) * lax.rsqrt(var + 1e-5) * gamma + beta).astype(jnp.bfloat16)


def reference(x, gamma, beta, wqkv, wo, w1, w2):
    hpg = HEADS // KV
    ntok = B * S
    ln = layer_norm(x, gamma, beta).reshape(ntok, D)
    qkv = jnp.dot(ln, wqkv, preferred_element_type=jnp.float32).astype(jnp.bfloat16)
    qkv = qkv.reshape(B, S, KV, hpg + 2, HEAD)
    pos = jnp.arange(S)
    causal = pos[:, None] >= pos[None, :]
    scale = HEAD ** -0.5

    def one_group(args):
        q, k, v = args
        sc = jnp.einsum('shd,td->hst', q.astype(jnp.float32), k.astype(jnp.float32)) * scale
        sc = jnp.where(causal[None], sc, -1e30)
        p = jax.nn.softmax(sc, axis=-1).astype(jnp.bfloat16)
        o = jnp.einsum('hst,td->shd', p.astype(jnp.float32), v.astype(jnp.float32))
        return o.astype(jnp.bfloat16)

    def one_seq(qkv_b):
        g = jnp.moveaxis(qkv_b, 1, 0)
        o = lax.map(one_group, (g[:, :, :hpg], g[:, :, hpg], g[:, :, hpg + 1]))
        return jnp.moveaxis(o, 0, 1).reshape(S, HEADS * HEAD)

    o = lax.map(one_seq, qkv).reshape(ntok, HEADS * HEAD)
    a = jnp.dot(o, wo.reshape(HEADS * HEAD, D), preferred_element_type=jnp.float32)
    hmid = jax.nn.gelu(jnp.dot(ln, w1, preferred_element_type=jnp.float32), approximate=False).astype(jnp.bfloat16)
    m = jnp.dot(hmid, w2, preferred_element_type=jnp.float32)
    upd = (a + m).astype(jnp.bfloat16).astype(jnp.float32).reshape(B, S, D)
    return (x.astype(jnp.float32) + upd).astype(jnp.bfloat16)
```

```python
import functools
import math

import jax
import jax.numpy as jnp
from jax import lax
from jax.experimental import pallas as pl
from jax.experimental.pallas import tpu as pltpu
from jax.sharding import PartitionSpec as P

BF = jnp.bfloat16
F32 = jnp.float32
DEPTH = 4
RING = 10
LAST = 11
CHANNELS = 13
COMM = True


def kernel(cfg, x, gamma, beta, wqkv, wo, w1, w2, y,
           wbuf, ln, qb, kc, vc, hbuf, part, xbuf, sb0, sb1, pb, mt0, mt1, s1r, r1l, r1r, r2l, r2r, ybuf, xp,
           wsem, xsem, ssem, rsem, ysem, xpsem):
    (ntok, d, s, hl, dh, f, tc, tp) = cfg
    sb, mt = (sb0, sb1), (mt0, mt1)
    hd = hl * dh
    chunks, per_seq = ntok // tc, s // tc
    nk = 8
    nb, dw, gw = d // nk, d // 4, f // 2
    qw = 3 * hd
    qa = (qw // 2 + 255) // 256 * 256
    th, to = tc // 2, tc // tp
    half = to // 2
    lnr = tc // 4
    nblk = chunks * nk
    nx = tp // 2

    me = lax.axis_index("tp")
    cx, q = me // 2, me % 2
    right = {"tp": ((cx + 1) % nx) * 2 + q}
    left = {"tp": ((cx + nx - 1) % nx) * 2 + q}
    partner = {"tp": cx * 2 + 1 - q}
    o_me = q * th + cx * to
    o_right = q * th + ((cx + 1) % nx) * to
    o_left = q * th + ((cx + nx - 1) % nx) * to
    o_opp = q * th + ((cx + 2) % nx) * to
    mine, theirs = q * th, (1 - q) * th

    def rows(start, size):
        return pl.ds(pl.multiple_of(start, math.gcd(size, half)), size)

    def wload(step, slot, i=None):
        if step == "q0":
            return [pltpu.make_async_copy(wqkv.at[:, 0:qa], wbuf.at[slot, 0:d, 0:qa], wsem.at[slot, 0])]
        if step == "q1":
            return [pltpu.make_async_copy(wqkv.at[:, qa:qw], wbuf.at[slot, 0:d, 0:qw - qa], wsem.at[slot, 0])]
        if step == "g":
            return [pltpu.make_async_copy(w1.at[:, pl.ds(pl.multiple_of(i * gw, 128), gw)], wbuf.at[slot, 0:d, 0:gw], wsem.at[slot, 0])]
        cols = pl.ds(pl.multiple_of(i * dw, 128), dw)
        return [pltpu.make_async_copy(w2.at[:, cols], wbuf.at[slot, 0:f, 0:dw], wsem.at[slot, 0]),
                pltpu.make_async_copy(wo.at[:, cols], wbuf.at[slot, f:f + hd, 0:dw], wsem.at[slot, 1])]

    def start(copies):
        for copy in copies:
            copy.start()

    def wait(copies):
        for copy in copies:
            copy.wait()

    def gather(tiles):
        return jnp.concatenate([tiles[:, g].reshape(tc, 128) for g in range(tiles.shape[1])], axis=1)

    def scatter(tiles, first, val):
        for g in range(val.shape[1] // 128):
            tiles[:, first + g] = val[:, g * 128:(g + 1) * 128].reshape(tc // 16, 16, 128)

    def xload(c, i):
        return pltpu.make_async_copy(x.at[pl.ds(pl.multiple_of(c * tc + i * lnr, lnr), lnr), :], xbuf.at[i % 2], xsem.at[i % 2])

    def norm(i):
        sub = 16
        for r in range(lnr // sub):
            xs = xbuf[i % 2, r * sub:(r + 1) * sub, :].astype(F32)
            xc = xs - jnp.sum(xs, axis=-1, keepdims=True) * (1.0 / d)
            inv = lax.rsqrt(jnp.sum(xc * xc, axis=-1, keepdims=True) * (1.0 / d) + 1e-5)
            out = (xc * inv * gamma[...] + beta[...]).astype(BF)
            for g in range(d // 128):
                ln[i * (lnr // sub) + r, g] = out[:, g * 128:(g + 1) * 128]

    def k(b):
        return lax.rem(b + 16, DEPTH)

    def ring(b):
        return lax.rem(b + 2 * RING, RING)

    def safe(b, i, spare):
        return jnp.where(b >= 0, i, spare)

    def y_at(b, off, size):
        c, kk = b // nk, b % nk
        return y.at[rows(c * tc + off, size), pl.ds(pl.multiple_of(kk * nb, 128), nb)]

    def remote(ch, b, src, dst, dev):
        return pltpu.make_async_remote_copy(src, dst, ssem.at[ch, k(b)], rsem.at[ch, k(b)], device_id=dev, device_id_type=pl.DeviceIdType.MESH)

    def t_pair(b):
        return [remote(0, b, part.at[ring(b), rows(theirs, th), :], s1r.at[lax.rem(b + 16, 2)], partner)]

    def t_first(b):
        p = ring(b)
        return [remote(1, b, part.at[p, rows(o_opp, half), :], r1l.at[k(b)], right),
                remote(2, b, part.at[p, rows(o_opp + half, half), :], r1r.at[k(b)], left)]

    def t_second(b):
        p = ring(b)
        return [remote(3, b, part.at[p, rows(o_right, to), :], r2l.at[k(b)], right),
                remote(4, b, part.at[p, rows(o_left, to), :], r2r.at[k(b)], left)]

    def t_own(b):
        src, dst = ybuf.at[k(b)], y_at(b, o_me, to)
        return [remote(5, b, src, dst, right), remote(6, b, src, dst, left), remote(7, b, src, dst, partner)]

    def t_keep(b):
        return pltpu.make_async_copy(ybuf.at[k(b)], y_at(b, o_me, to), ysem.at[k(b)])

    def t_pass(b):
        a, z = y_at(b, o_left, half), y_at(b, o_right + half, half)
        l, r = y_at(b, o_left, to), y_at(b, o_right, to)
        return [remote(8, b, a, a, right), remote(9, b, z, z, left), remote(10, b, l, l, partner), remote(11, b, r, r, partner)]

    def t_opp(b):
        o = y_at(b, o_opp, to)
        return [remote(12, b, o, o, partner)]

    def t_x(b):
        c, kk = b // nk, b % nk
        return pltpu.make_async_copy(x.at[rows(c * tc + o_me, to), pl.ds(pl.multiple_of(kk * nb, 128), nb)], xp.at[k(b)], xpsem.at[k(b)])

    def drain(copies):
        for copy in copies:
            copy.wait_recv()
            copy.wait_send()

    def waits(n, on):
        on(n - 1, lambda b: drain(t_pair(b)))
        on(n - 3, lambda b: drain(t_first(b)))
        on(n - 5, lambda b: (drain(t_second(b)), t_x(b).wait()))
        on(n - 7, lambda b: (drain(t_own(b)), t_keep(b).wait()))
        on(n - 9, lambda b: drain(t_pass(b)))
        on(n - LAST, lambda b: drain(t_opp(b)))

    def sends(n, on):
        on(n - 9, lambda b: start(t_opp(b)))
        on(n - 7, lambda b: start(t_pass(b)))
        on(n - 5, lambda b: (start(t_own(b)), t_keep(b).start()))
        on(n - 3, lambda b: (start(t_second(b)), t_x(b).start()))
        on(n - 1, lambda b: start(t_first(b)))
        on(n, lambda b: start(t_pair(b)))

    def sum_pair(b, p, i):
        at = rows(mine, th)
        part[p, at, :] = part[p, at, :] + s1r[i]

    def sum_first(b, p, i):
        at = rows(o_right, half)
        part[p, at, :] = part[p, at, :] + r1l[i]
        at = rows(o_left + half, half)
        part[p, at, :] = part[p, at, :] + r1r[i]

    def sum_second(b, p, i):
        u = part[p, rows(o_me, to), :].astype(F32) + (r2l[i].astype(F32) + r2r[i].astype(F32))
        ybuf[k(b)] = (xp[i].astype(F32) + u.astype(BF).astype(F32)).astype(BF)

    def adds(n):
        for delta, f_ in ((1, sum_pair), (3, sum_first), (5, sum_second)):
            b = n - delta
            f_(b, ring(b), safe(b, lax.rem(b + 16, 2), 2) if delta == 1 else safe(b, k(b), DEPTH))

    def guarded(cond, b, g):
        @pl.when(cond)
        def _():
            g(b)

    def when_at_least(n, f_):
        hot = n >= LAST

        @pl.when(hot)
        def _():
            f_(n, lambda b, g: g(b))

        @pl.when(jnp.logical_not(hot))
        def _():
            f_(n, lambda b, g: guarded(b >= 0, b, g))

    def step(n, compute):
        if COMM:
            when_at_least(n, waits)
            adds(n)
        compute()
        if COMM:
            when_at_least(n, sends)

    def put_qkv(c, r, first):
        base = pl.multiple_of(lax.rem(c, per_seq) * tc, tc)
        for i in range(r.shape[1] // dh):
            head, kind = divmod(first // dh + i, 3)
            val = r[:, i * dh:(i + 1) * dh].astype(BF)
            if kind == 0:
                qb[head] = val
            else:
                (kc, vc)[kind - 1][head, pl.ds(base, tc), :] = val

    def attend(c):
        scale = dh ** -0.5 * math.log2(math.e)
        j = lax.rem(c, per_seq)
        qr = tc // 2
        block = min(64, qr)
        blocks = [slice(r, r + block) for r in range(0, qr, block)]

        def scores(h, i, tiles):
            width = (tiles - 1) * tc + (i + 1) * qr
            m = None
            for lo in range(0, width, tc):
                hi = min(lo + tc, width)
                st = lax.dot_general(qb[h, i * qr:(i + 1) * qr, :], kc[h, lo:hi, :], (((1,), (1,)), ((), ())), preferred_element_type=F32)
                if hi == width:
                    row = lax.broadcasted_iota(jnp.int32, st.shape, 0) + i * qr
                    st = jnp.where(row >= lax.broadcasted_iota(jnp.int32, st.shape, 1), st, -1e30)
                sb[i][:, lo:hi] = st
                for g in range(0, hi - lo, 128):
                    v = st[:, g:g + 128]
                    m = v if m is None else jnp.maximum(m, v)
            mt[i][...] = m

        def output(h, i, tiles):
            width = (tiles - 1) * tc + (i + 1) * qr
            sums = []
            for rb in blocks:
                top = jnp.max(mt[i][rb], axis=1, keepdims=True)
                e = jnp.exp2((sb[i][rb, 0:width] - top) * scale)
                sums.append(jnp.sum(e, axis=1, keepdims=True))
                e = e.astype(BF)
                for g in range(width // 128):
                    pb[i, rb.start // 16:rb.stop // 16, g] = e[:, g * 128:(g + 1) * 128].reshape(block // 16, 16, 128)
            p = jnp.concatenate([pb[i, :, g].reshape(qr, 128) for g in range(width // 128)], axis=1)
            o = jnp.dot(p, vc[h, 0:width, :], preferred_element_type=F32)
            for rb, total in zip(blocks, sums):
                first = (i * qr + rb.start) // 16
                hbuf[first:first + block // 16, f // 128 + h] = (o[rb] / total).astype(BF).reshape(block // 16, 16, 128)

        for tiles in range(1, per_seq + 1):
            @pl.when(j == tiles - 1)
            def _(tiles=tiles):
                scores(0, 0, tiles)

                @pl.loop(0, hl)
                def _(h):
                    scores(h, 1, tiles)
                    output(h, 0, tiles)
                    scores(jnp.minimum(h + 1, hl - 1), 0, tiles)
                    output(h, 1, tiles)

    def gelu(r):
        return 0.5 * r * (1.0 + lax.erf(r * (0.5 ** 0.5)))

    start(wload("q0", 0))
    xload(0, 0).start()
    if COMM:
        barrier = pltpu.get_barrier_semaphore()
        for dev in (partner, right, left):
            pl.semaphore_signal(barrier, inc=1, device_id=dev, device_id_type=pl.DeviceIdType.MESH)
        pl.semaphore_wait(barrier, 3)

    @pl.loop(0, 4)
    def _(i):
        @pl.when(i < 3)
        def _():
            xload(0, i + 1).start()
        xload(0, i).wait()
        norm(i)

    @pl.loop(0, chunks)
    def _(c):
        n0 = c * nk - 4
        nxt = jnp.minimum(c + 1, chunks - 1)

        wait(wload("q0", 0))
        start(wload("q1", 1))

        def q0():
            put_qkv(c, jnp.dot(gather(ln), wbuf[0, 0:d, 0:qa], preferred_element_type=F32), 0)
        step(n0, q0)

        wait(wload("q1", 1))
        start(wload("g", 0, 0))

        def q1():
            put_qkv(c, jnp.dot(gather(ln), wbuf[1, 0:d, 0:qw - qa], preferred_element_type=F32), qa)
        step(n0 + 1, q1)

        attend(c)

        @pl.loop(0, 2)
        def _(i):
            wait(wload("g", i, i))

            @pl.when(i == 0)
            def _():
                start(wload("g", 1, 1))

            @pl.when(i == 1)
            def _():
                start(wload("d", 0, 0))
                xload(nxt, 0).start()

            def g():
                r = jnp.dot(gather(ln), wbuf[i, 0:d, 0:gw], preferred_element_type=F32)
                scatter(hbuf, i * (gw // 128), gelu(r).astype(BF))
            step(n0 + 2 + i, g)

        @pl.loop(0, 4)
        def _(i):
            slot = lax.rem(i, 2)
            wait(wload("d", slot, i))
            xload(nxt, i).wait()

            @pl.when(i < 3)
            def _():
                start(wload("d", 1 - slot, i + 1))
                xload(nxt, i + 1).start()

            @pl.when(jnp.logical_and(i == 3, c < chunks - 1))
            def _():
                start(wload("q0", 0))

            def dd():
                norm(i)
                r = jnp.dot(gather(hbuf), wbuf[slot, 0:f + hd, 0:dw], preferred_element_type=F32)
                b = c * nk + 2 * i
                part[ring(b)] = r[:, 0:nb].astype(BF)
                part[ring(b + 1)] = r[:, nb:2 * nb].astype(BF)
            step(n0 + 4 + i, dd)

    if COMM:
        @pl.loop(nblk - 4, nblk + LAST)
        def _(n):
            def on(b, g):
                guarded(b < nblk, b, g)
            waits(n, on)
            for delta, f_ in ((1, sum_pair), (3, sum_first), (5, sum_second)):
                on(n - delta, lambda b, f_=f_, w=2 if delta == 1 else DEPTH: f_(b, ring(b), lax.rem(b, w)))
            sends(n, on)


def layer(cfg, x, gamma, beta, wqkv, wo, w1, w2):
    (ntok, d, s, hl, dh, f, tc, tp) = cfg
    nb, to = d // 8, tc // tp
    any_ = pl.BlockSpec(memory_space=pl.ANY)
    vm = pl.BlockSpec(memory_space=pltpu.VMEM)
    qw = 3 * hl * dh
    qa = (qw // 2 + 255) // 256 * 256
    width = max(qa, qw - qa, f // 2, d // 4)
    depth = max(d, f + hl * dh)
    return pl.pallas_call(
        functools.partial(kernel, cfg),
        out_shape=jax.ShapeDtypeStruct((ntok, d), BF),
        in_specs=[any_, vm, vm, any_, any_, any_, any_],
        out_specs=any_,
        scratch_shapes=[
            pltpu.VMEM((2, depth, width), BF),
            pltpu.VMEM((tc // 16, d // 128, 16, 128), BF),
            pltpu.VMEM((hl, tc, dh), BF),
            pltpu.VMEM((hl, s, dh), BF),
            pltpu.VMEM((hl, s, dh), BF),
            pltpu.VMEM((tc // 16, (f + hl * dh) // 128, 16, 128), BF),
            pltpu.VMEM((RING, tc, nb), BF),
            pltpu.VMEM((2, tc // 4, d), BF),
            pltpu.VMEM((tc // 2, s), F32),
            pltpu.VMEM((tc // 2, s), F32),
            pltpu.VMEM((2, tc // 32, s // 128, 16, 128), BF),
            *[pltpu.VMEM((tc // 2, 128), F32) for _ in range(2)],
            pltpu.VMEM((3, tc // 2, nb), BF),
            pltpu.VMEM((DEPTH + 1, to // 2, nb), BF),
            pltpu.VMEM((DEPTH + 1, to // 2, nb), BF),
            pltpu.VMEM((DEPTH + 1, to, nb), BF),
            pltpu.VMEM((DEPTH + 1, to, nb), BF),
            pltpu.VMEM((DEPTH, to, nb), BF),
            pltpu.VMEM((DEPTH + 1, to, nb), BF),
            pltpu.SemaphoreType.DMA((2, 2)),
            pltpu.SemaphoreType.DMA((2,)),
            pltpu.SemaphoreType.DMA((CHANNELS, DEPTH)),
            pltpu.SemaphoreType.DMA((CHANNELS, DEPTH)),
            pltpu.SemaphoreType.DMA((DEPTH,)),
            pltpu.SemaphoreType.DMA((DEPTH,)),
        ],
        compiler_params=pltpu.CompilerParams(
            collective_id=0 if COMM else None, has_side_effects=True, vmem_limit_bytes=67043328),
        name="layer",
    )(x, gamma, beta, wqkv, wo, w1, w2)


def solution(mesh):
    tp = mesh.shape["tp"]

    def local(x, gamma, beta, wqkv, wo, w1, w2):
        b, s, d = x.shape
        hl, dh, _ = wo.shape
        cfg = (b * s, d, s, hl, dh, w1.shape[1], s // 4, tp)
        y = layer(cfg, x.reshape(b * s, d), gamma.reshape(1, d), beta.reshape(1, d),
                  wqkv, wo.reshape(hl * dh, d), w1, w2)
        return y.reshape(b, s, d)

    return jax.shard_map(local, mesh=mesh,
                         in_specs=(P('dp', None, None), P(None), P(None), P(None, 'tp'),
                                   P('tp', None, None), P(None, 'tp'), P('tp', None)),
                         out_specs=P('dp', None, None), check_vma=False)
```

```python
import functools
import math

import jax
import jax.numpy as jnp
from jax import lax
from jax.experimental import pallas as pl
from jax.experimental.pallas import tpu as pltpu
from jax.sharding import PartitionSpec as P

BF = jnp.bfloat16
F32 = jnp.float32
DEPTH = 4
RING = 10
LAST = 11
CHANNELS = 6
COMM = True


def kernel(cfg, x, gamma, beta, wqkv, wo, w1, w2, y,
           wbuf, ln, qb, kc, vc, hbuf, part, xbuf, sb0, sb1, pb, mt0, mt1, s1r, r1l, r1r, r2l, r2r, ybuf, xp,
           wsem, xsem, ssem, rsem, ysem, xpsem):
    (ntok, d, s, hl, dh, f, tc, tp) = cfg
    sb, mt = (sb0, sb1), (mt0, mt1)
    hd = hl * dh
    chunks, per_seq = ntok // tc, s // tc
    nk = 8
    nb, dw, gw = d // nk, d // 4, f // 2
    qw = 3 * hd
    qa = (qw // 2 + 255) // 256 * 256
    th, to = tc // 2, tc // tp
    half = to // 2
    lnr = tc // 4
    nblk = chunks * nk
    nx = tp // 2

    me = lax.axis_index("tp")
    cx, q = me // 2, me % 2
    right = {"tp": ((cx + 1) % nx) * 2 + q}
    left = {"tp": ((cx + nx - 1) % nx) * 2 + q}
    partner = {"tp": cx * 2 + 1 - q}
    o_me = q * th + cx * to
    o_right = q * th + ((cx + 1) % nx) * to
    o_left = q * th + ((cx + nx - 1) % nx) * to
    o_opp = q * th + ((cx + 2) % nx) * to
    mine, theirs = q * th, (1 - q) * th

    def rows(start, size):
        return pl.ds(pl.multiple_of(start, math.gcd(size, half)), size)

    def wload(step, slot, i=None):
        if step == "q0":
            return [pltpu.make_async_copy(wqkv.at[:, 0:qa], wbuf.at[slot, 0:d, 0:qa], wsem.at[slot, 0])]
        if step == "q1":
            return [pltpu.make_async_copy(wqkv.at[:, qa:qw], wbuf.at[slot, 0:d, 0:qw - qa], wsem.at[slot, 0])]
        if step == "g":
            return [pltpu.make_async_copy(w1.at[:, pl.ds(pl.multiple_of(i * gw, 128), gw)], wbuf.at[slot, 0:d, 0:gw], wsem.at[slot, 0])]
        cols = pl.ds(pl.multiple_of(i * dw, 128), dw)
        return [pltpu.make_async_copy(w2.at[:, cols], wbuf.at[slot, 0:f, 0:dw], wsem.at[slot, 0]),
                pltpu.make_async_copy(wo.at[:, cols], wbuf.at[slot, f:f + hd, 0:dw], wsem.at[slot, 1])]

    def start(copies):
        for copy in copies:
            copy.start()

    def wait(copies):
        for copy in copies:
            copy.wait()

    def gather(tiles, corner=None):
        parts = [tiles[:, g].reshape(tc, 128) for g in range(tiles.shape[1])]
        if corner:
            parts[0] = jnp.concatenate([corner(parts[0][:8]), parts[0][8:]], axis=0)
        return jnp.concatenate(parts, axis=1)

    def scatter(tiles, first, val):
        for g in range(val.shape[1] // 128):
            tiles[:, first + g] = val[:, g * 128:(g + 1) * 128].reshape(tc // 16, 16, 128)

    def xload(c, i):
        return pltpu.make_async_copy(x.at[pl.ds(pl.multiple_of(c * tc + i * lnr, lnr), lnr), :], xbuf.at[i % 2], xsem.at[i % 2])

    def norm(i):
        sub = 8
        seen = None
        for r in range(lnr // sub):
            xs = xbuf[i % 2, r * sub:(r + 1) * sub, :].astype(F32)
            xc = xs - jnp.sum(xs, axis=-1, keepdims=True) * (1.0 / d)
            inv = lax.rsqrt(jnp.sum(xc * xc, axis=-1, keepdims=True) * (1.0 / d) + 1e-5)
            out = (xc * inv * gamma[...] + beta[...]).astype(BF)
            for g in range(d // 128):
                v = out[:, g * 128:(g + 1) * 128]
                ln[i * (lnr // 16) + r // 2, g, r % 2 * 8:r % 2 * 8 + 8] = v
                seen = v if seen is None else jnp.maximum(seen, v)
        return seen

    def k(b):
        return lax.rem(b + 16, DEPTH)

    def ring(b):
        return lax.rem(b + 2 * RING, RING)

    def y_at(b, off, size):
        c, kk = b // nk, b % nk
        return y.at[rows(c * tc + off, size), pl.ds(pl.multiple_of(kk * nb, 128), nb)]

    def remote(ch, b, src, dst, dev):
        return pltpu.make_async_remote_copy(src, dst, ssem.at[ch, k(b)], rsem.at[ch, k(b)], device_id=dev, device_id_type=pl.DeviceIdType.MESH)

    def t_pair(b):
        return [remote(0, b, part.at[ring(b), rows(theirs, th), :], s1r.at[lax.rem(b + 16, 2)], partner)]

    def t_first(b):
        p = ring(b)
        return [remote(1, b, part.at[p, rows(o_opp, half), :], r1l.at[k(b)], right),
                remote(1, b, part.at[p, rows(o_opp + half, half), :], r1r.at[k(b)], left)]

    def t_second(b):
        p = ring(b)
        return [remote(2, b, part.at[p, rows(o_right, to), :], r2l.at[k(b)], right),
                remote(2, b, part.at[p, rows(o_left, to), :], r2r.at[k(b)], left)]

    def t_own(b):
        src, dst = ybuf.at[k(b)], y_at(b, o_me, to)
        return [remote(3, b, src, dst, right), remote(3, b, src, dst, left)]

    def t_keep(b):
        return pltpu.make_async_copy(ybuf.at[k(b)], y_at(b, o_me, to), ysem.at[k(b)])

    def t_pass(b):
        a, z = y_at(b, o_left, half), y_at(b, o_right + half, half)
        return [remote(4, b, a, a, right), remote(4, b, z, z, left)]

    def t_half(b):
        o = y_at(b, mine, th)
        return [remote(5, b, o, o, partner)]

    def t_x(b):
        c, kk = b // nk, b % nk
        return pltpu.make_async_copy(x.at[rows(c * tc + o_me, to), pl.ds(pl.multiple_of(kk * nb, 128), nb)], xp.at[k(b)], xpsem.at[k(b)])

    def drain(ch, b, size):
        ref = part.at[0, 0:size, :]
        copy = remote(ch, b, ref, ref, partner)
        copy.wait_recv()
        copy.wait_send()

    def sum_pair(b):
        p, at = ring(b), rows(mine, th)
        part[p, at, :] = part[p, at, :] + s1r[lax.rem(b + 16, 2)]

    def sum_first(b):
        p = ring(b)
        at = rows(o_right, half)
        part[p, at, :] = part[p, at, :] + r1l[k(b)]
        at = rows(o_left + half, half)
        part[p, at, :] = part[p, at, :] + r1r[k(b)]

    def sum_second(b):
        u = part[ring(b), rows(o_me, to), :].astype(F32) + (r2l[k(b)].astype(F32) + r2r[k(b)].astype(F32))
        ybuf[k(b)] = (xp[k(b)].astype(F32) + u.astype(BF).astype(F32)).astype(BF)

    def pump(n, on):
        on(n - 1, lambda b: drain(0, b, th))
        on(n - 3, lambda b: drain(1, b, to))
        on(n - 5, lambda b: (drain(2, b, 2 * to), t_x(b).wait()))
        on(n - 7, lambda b: (drain(3, b, 2 * to), t_keep(b).wait()))
        on(n - 9, lambda b: drain(4, b, to))
        on(n - LAST, lambda b: drain(5, b, th))
        on(n - 3, sum_first)
        on(n - 5, sum_second)
        on(n - 1, sum_pair)
        on(n - 3, lambda b: (start(t_second(b)), t_x(b).start()))
        on(n - 5, lambda b: (start(t_own(b)), t_keep(b).start()))
        on(n - 1, lambda b: start(t_first(b)))
        on(n - 7, lambda b: start(t_pass(b)))
        on(n, lambda b: start(t_pair(b)))
        on(n - 9, lambda b: start(t_half(b)))

    def guarded(cond, b, g):
        @pl.when(cond)
        def _():
            g(b)

    def step(n):
        if COMM:
            @pl.when(n >= LAST)
            def _():
                pump(n, lambda b, g: g(b) and None)

            @pl.when(n < LAST)
            def _():
                pump(n, lambda b, g: guarded(b >= 0, b, g))

    def put_qkv(c, r, first):
        base = pl.multiple_of(lax.rem(c, per_seq) * tc, tc)
        for i in range(r.shape[1] // dh):
            head, kind = divmod(first // dh + i, 3)
            val = r[:, i * dh:(i + 1) * dh].astype(BF)
            if kind == 0:
                qb[head] = val
            else:
                (kc, vc)[kind - 1][head, pl.ds(base, tc), :] = val

    def attend(c):
        scale = dh ** -0.5 * math.log2(math.e)
        j = lax.rem(c, per_seq)
        qr = tc // 2
        block = min(64, qr)
        blocks = [slice(r, r + block) for r in range(0, qr, block)]

        def scores(h, i, tiles):
            width = (tiles - 1) * tc + (i + 1) * qr
            m = None
            for lo in range(0, width, tc):
                hi = min(lo + tc, width)
                st = lax.dot_general(qb[h, i * qr:(i + 1) * qr, :], kc[h, lo:hi, :], (((1,), (1,)), ((), ())), preferred_element_type=F32)
                if hi == width:
                    row = lax.broadcasted_iota(jnp.int32, st.shape, 0) + i * qr
                    st = jnp.where(row >= lax.broadcasted_iota(jnp.int32, st.shape, 1), st, -1e30)
                sb[i][:, lo:hi] = st
                for g in range(0, hi - lo, 128):
                    v = st[:, g:g + 128]
                    m = v if m is None else jnp.maximum(m, v)
            mt[i][...] = m

        def output(h, i, tiles):
            width = (tiles - 1) * tc + (i + 1) * qr
            sums = []
            for rb in blocks:
                top = jnp.max(mt[i][rb], axis=1, keepdims=True)
                e = jnp.exp2((sb[i][rb, 0:width] - top) * scale)
                sums.append(jnp.sum(e, axis=1, keepdims=True))
                e = e.astype(BF)
                for g in range(width // 128):
                    pb[i, rb.start // 16:rb.stop // 16, g] = e[:, g * 128:(g + 1) * 128].reshape(block // 16, 16, 128)
            p = jnp.concatenate([pb[i, :, g].reshape(qr, 128) for g in range(width // 128)], axis=1)
            o = jnp.dot(p, vc[h, 0:width, :], preferred_element_type=F32)
            for rb, total in zip(blocks, sums):
                first = (i * qr + rb.start) // 16
                hbuf[first:first + block // 16, f // 128 + h] = (o[rb] / total).astype(BF).reshape(block // 16, 16, 128)

        for tiles in range(1, per_seq + 1):
            @pl.when(j == tiles - 1)
            def _(tiles=tiles):
                scores(0, 0, tiles)

                @pl.loop(0, hl)
                def _(h):
                    scores(h, 1, tiles)
                    output(h, 0, tiles)
                    scores(jnp.minimum(h + 1, hl - 1), 0, tiles)
                    output(h, 1, tiles)

    def gelu(r):
        return 0.5 * r * (1.0 + lax.erf(r * (0.5 ** 0.5)))

    start(wload("q0", 0))
    xload(0, 0).start()
    if COMM:
        barrier = pltpu.get_barrier_semaphore()
        for dev in (partner, right, left):
            pl.semaphore_signal(barrier, inc=1, device_id=dev, device_id_type=pl.DeviceIdType.MESH)
        pl.semaphore_wait(barrier, 3)

    @pl.loop(0, 4)
    def _(i):
        @pl.when(i < 3)
        def _():
            xload(0, i + 1).start()
        xload(0, i).wait()
        norm(i)

    @pl.loop(0, chunks)
    def _(c):
        n0 = c * nk - 5
        nxt = jnp.minimum(c + 1, chunks - 1)

        step(n0)
        wait(wload("q0", 0))
        start(wload("q1", 1))
        put_qkv(c, jnp.dot(gather(ln), wbuf[0, 0:d, 0:qa], preferred_element_type=F32), 0)

        step(n0 + 1)
        wait(wload("q1", 1))
        start(wload("g", 0, 0))
        put_qkv(c, jnp.dot(gather(ln), wbuf[1, 0:d, 0:qw - qa], preferred_element_type=F32), qa)

        attend(c)

        @pl.loop(0, 2)
        def _(i):
            step(n0 + 2 + i)
            wait(wload("g", i, i))

            @pl.when(i == 0)
            def _():
                start(wload("g", 1, 1))

            @pl.when(i == 1)
            def _():
                start(wload("d", 0, 0))
                xload(nxt, 0).start()

            r = jnp.dot(gather(ln), wbuf[i, 0:d, 0:gw], preferred_element_type=F32)
            scatter(hbuf, i * (gw // 128), gelu(r).astype(BF))

        @pl.loop(0, 4)
        def _(i):
            slot = lax.rem(i, 2)
            step(n0 + 4 + i)
            wait(wload("d", slot, i))
            xload(nxt, i).wait()

            @pl.when(i < 3)
            def _():
                start(wload("d", 1 - slot, i + 1))
                xload(nxt, i + 1).start()

            @pl.when(jnp.logical_and(i == 3, c < chunks - 1))
            def _():
                start(wload("q0", 0))

            b = c * nk + 2 * i
            cut = (dw // 2 + 255) // 256 * 256
            seen = norm(i)
            tiles = gather(hbuf)
            r0 = jnp.dot(tiles, wbuf[slot, 0:f + hd, 0:cut], preferred_element_type=F32)
            tiles = gather(hbuf, lambda v: jnp.where(me < 0, seen, v))
            r1 = jnp.dot(tiles, wbuf[slot, 0:f + hd, cut:dw], preferred_element_type=F32)
            part[ring(b)] = r0[:, 0:nb].astype(BF)
            part[ring(b + 1), :, 0:cut - nb] = r0[:, nb:cut].astype(BF)
            part[ring(b + 1), :, cut - nb:nb] = r1.astype(BF)

    if COMM:
        @pl.loop(nblk - 5, nblk + LAST)
        def _(n):
            pump(n, lambda b, g: guarded(b < nblk, b, g))


def layer(cfg, x, gamma, beta, wqkv, wo, w1, w2):
    (ntok, d, s, hl, dh, f, tc, tp) = cfg
    nb, to = d // 8, tc // tp
    any_ = pl.BlockSpec(memory_space=pl.ANY)
    vm = pl.BlockSpec(memory_space=pltpu.VMEM)
    qw = 3 * hl * dh
    qa = (qw // 2 + 255) // 256 * 256
    width = max(qa, qw - qa, f // 2, d // 4)
    depth = max(d, f + hl * dh)
    return pl.pallas_call(
        functools.partial(kernel, cfg),
        out_shape=jax.ShapeDtypeStruct((ntok, d), BF),
        in_specs=[any_, vm, vm, any_, any_, any_, any_],
        out_specs=any_,
        scratch_shapes=[
            pltpu.VMEM((2, depth, width), BF),
            pltpu.VMEM((tc // 16, d // 128, 16, 128), BF),
            pltpu.VMEM((hl, tc, dh), BF),
            pltpu.VMEM((hl, s, dh), BF),
            pltpu.VMEM((hl, s, dh), BF),
            pltpu.VMEM((tc // 16, (f + hl * dh) // 128, 16, 128), BF),
            pltpu.VMEM((RING, tc, nb), BF),
            pltpu.VMEM((2, tc // 4, d), BF),
            pltpu.VMEM((tc // 2, s), F32),
            pltpu.VMEM((tc // 2, s), F32),
            pltpu.VMEM((2, tc // 32, s // 128, 16, 128), BF),
            *[pltpu.VMEM((tc // 2, 128), F32) for _ in range(2)],
            pltpu.VMEM((2, tc // 2, nb), BF),
            pltpu.VMEM((DEPTH, to // 2, nb), BF),
            pltpu.VMEM((DEPTH, to // 2, nb), BF),
            pltpu.VMEM((DEPTH, to, nb), BF),
            pltpu.VMEM((DEPTH, to, nb), BF),
            pltpu.VMEM((DEPTH, to, nb), BF),
            pltpu.VMEM((DEPTH, to, nb), BF),
            pltpu.SemaphoreType.DMA((2, 2)),
            pltpu.SemaphoreType.DMA((2,)),
            pltpu.SemaphoreType.DMA((CHANNELS, DEPTH)),
            pltpu.SemaphoreType.DMA((CHANNELS, DEPTH)),
            pltpu.SemaphoreType.DMA((DEPTH,)),
            pltpu.SemaphoreType.DMA((DEPTH,)),
        ],
        compiler_params=pltpu.CompilerParams(
            collective_id=0 if COMM else None, has_side_effects=True, vmem_limit_bytes=67043328),
        name="layer",
    )(x, gamma, beta, wqkv, wo, w1, w2)


def solution(mesh):
    tp = mesh.shape["tp"]

    def local(x, gamma, beta, wqkv, wo, w1, w2):
        b, s, d = x.shape
        hl, dh, _ = wo.shape
        cfg = (b * s, d, s, hl, dh, w1.shape[1], s // 4, tp)
        y = layer(cfg, x.reshape(b * s, d), gamma.reshape(1, d), beta.reshape(1, d),
                  wqkv, wo.reshape(hl * dh, d), w1, w2)
        return y.reshape(b, s, d)

    return jax.shard_map(local, mesh=mesh,
                         in_specs=(P('dp', None, None), P(None), P(None), P(None, 'tp'),
                                   P('tp', None, None), P(None, 'tp'), P('tp', None)),
                         out_specs=P('dp', None, None), check_vma=False)
```

```python
import functools
import math

import jax
import jax.numpy as jnp
from jax import lax
from jax.experimental import pallas as pl
from jax.experimental.pallas import tpu as pltpu
from jax.sharding import PartitionSpec as P

BF = jnp.bfloat16
F32 = jnp.float32
DEPTH = 4
RING = 10
LAST = 11
CHANNELS = 6
COMM = True
UNROLL = 2


def kernel(cfg, x, gamma, beta, wqkv, wo, w1, w2, y,
           wbuf, ln, qb, kc, vc, hbuf, part, xbuf, sb0, sb1, pb0, pb1, mt0, mt1, s1r, r1l, r1r, r2l, r2r, ybuf, xp,
           wsem, xsem, ssem, rsem, ysem, xpsem):
    (ntok, d, s, hl, dh, f, tc, tp) = cfg
    sb, pb, mt = (sb0, sb1), (pb0, pb1), (mt0, mt1)
    hd = hl * dh
    chunks, per_seq = ntok // tc, s // tc
    nk = 8
    nb, dw, gw = d // nk, d // 4, f // 2
    qw = 3 * hd
    qa = (qw // 2 + 255) // 256 * 256
    th, to = tc // 2, tc // tp
    half = to // 2
    lnr = tc // 4
    nblk = chunks * nk
    nx = tp // 2

    me = lax.axis_index("tp")
    cx, q = me // 2, me % 2
    right = {"tp": ((cx + 1) % nx) * 2 + q}
    left = {"tp": ((cx + nx - 1) % nx) * 2 + q}
    partner = {"tp": cx * 2 + 1 - q}
    o_me = q * th + cx * to
    o_right = q * th + ((cx + 1) % nx) * to
    o_left = q * th + ((cx + nx - 1) % nx) * to
    o_opp = q * th + ((cx + 2) % nx) * to
    mine, theirs = q * th, (1 - q) * th

    def rows(start, size):
        return pl.ds(pl.multiple_of(start, math.gcd(size, half)), size)

    def wload(step, slot, i=None):
        if step == "q0":
            return [pltpu.make_async_copy(wqkv.at[:, 0:qa], wbuf.at[slot, 0:d, 0:qa], wsem.at[slot, 0])]
        if step == "q1":
            return [pltpu.make_async_copy(wqkv.at[:, qa:qw], wbuf.at[slot, 0:d, 0:qw - qa], wsem.at[slot, 0])]
        if step == "g":
            return [pltpu.make_async_copy(w1.at[:, pl.ds(pl.multiple_of(i * gw, 128), gw)], wbuf.at[slot, 0:d, 0:gw], wsem.at[slot, 0])]
        cols = pl.ds(pl.multiple_of(i * dw, 128), dw)
        return [pltpu.make_async_copy(w2.at[:, cols], wbuf.at[slot, 0:f, 0:dw], wsem.at[slot, 0]),
                pltpu.make_async_copy(wo.at[:, cols], wbuf.at[slot, f:f + hd, 0:dw], wsem.at[slot, 1])]

    def start(copies):
        for copy in copies:
            copy.start()

    def wait(copies):
        for copy in copies:
            copy.wait()

    def gather(tiles, corner=None):
        parts = [tiles[:, g].reshape(tc, 128) for g in range(tiles.shape[1])]
        if corner:
            parts[0] = jnp.concatenate([corner(parts[0][:8]), parts[0][8:]], axis=0)
        return jnp.concatenate(parts, axis=1)

    def scatter(tiles, first, val):
        for g in range(val.shape[1] // 128):
            tiles[:, first + g] = val[:, g * 128:(g + 1) * 128].reshape(tc // 16, 16, 128)

    def xload(c, i):
        return pltpu.make_async_copy(x.at[pl.ds(pl.multiple_of(c * tc + i * lnr, lnr), lnr), :], xbuf.at[i % 2], xsem.at[i % 2])

    def norm(i):
        sub = 8
        seen = None
        for r in range(lnr // sub):
            xs = xbuf[i % 2, r * sub:(r + 1) * sub, :].astype(F32)
            xc = xs - jnp.sum(xs, axis=-1, keepdims=True) * (1.0 / d)
            inv = lax.rsqrt(jnp.sum(xc * xc, axis=-1, keepdims=True) * (1.0 / d) + 1e-5)
            out = (xc * inv * gamma[...] + beta[...]).astype(BF)
            for g in range(d // 128):
                v = out[:, g * 128:(g + 1) * 128]
                ln[i * (lnr // 16) + r // 2, g, r % 2 * 8:r % 2 * 8 + 8] = v
                seen = v if seen is None else jnp.maximum(seen, v)
        return seen

    def k(b):
        return lax.rem(b + 16, DEPTH)

    def two(b):
        return lax.rem(b + 16, 2)

    def ring(b):
        return lax.rem(b + 2 * RING, RING)

    def y_at(b, off, size):
        c, kk = b // nk, b % nk
        return y.at[rows(c * tc + off, size), pl.ds(pl.multiple_of(kk * nb, 128), nb)]

    def remote(ch, b, src, dst, dev):
        return pltpu.make_async_remote_copy(src, dst, ssem.at[ch, k(b)], rsem.at[ch, k(b)], device_id=dev, device_id_type=pl.DeviceIdType.MESH)

    def t_pair(b):
        return [remote(0, b, part.at[ring(b), rows(theirs, th), :], s1r.at[two(b)], partner)]

    def t_first(b):
        p = ring(b)
        return [remote(1, b, part.at[p, rows(o_opp, half), :], r1l.at[k(b)], right),
                remote(1, b, part.at[p, rows(o_opp + half, half), :], r1r.at[k(b)], left)]

    def t_second(b):
        p = ring(b)
        return [remote(2, b, part.at[p, rows(o_right, to), :], r2l.at[k(b)], right),
                remote(2, b, part.at[p, rows(o_left, to), :], r2r.at[k(b)], left)]

    def t_own(b):
        src, dst = ybuf.at[two(b)], y_at(b, o_me, to)
        return [remote(3, b, src, dst, right), remote(3, b, src, dst, left)]

    def t_keep(b):
        return pltpu.make_async_copy(ybuf.at[two(b)], y_at(b, o_me, to), ysem.at[k(b)])

    def t_pass(b):
        a, z = y_at(b, o_left, half), y_at(b, o_right + half, half)
        return [remote(4, b, a, a, right), remote(4, b, z, z, left)]

    def t_half(b):
        o = y_at(b, mine, th)
        return [remote(5, b, o, o, partner)]

    def t_x(b):
        c, kk = b // nk, b % nk
        return pltpu.make_async_copy(x.at[rows(c * tc + o_me, to), pl.ds(pl.multiple_of(kk * nb, 128), nb)], xp.at[two(b)], xpsem.at[k(b)])

    def drain(ch, b, size):
        ref = part.at[0, 0:size, :]
        copy = remote(ch, b, ref, ref, partner)
        copy.wait_recv()
        copy.wait_send()

    def sum_pair(b):
        p, at = ring(b), rows(mine, th)
        part[p, at, :] = part[p, at, :] + s1r[two(b)]

    def sum_first(b):
        p = ring(b)
        at = rows(o_right, half)
        part[p, at, :] = part[p, at, :] + r1l[k(b)]
        at = rows(o_left + half, half)
        part[p, at, :] = part[p, at, :] + r1r[k(b)]

    def sum_second(b):
        u = part[ring(b), rows(o_me, to), :].astype(F32) + (r2l[k(b)].astype(F32) + r2r[k(b)].astype(F32))
        ybuf[two(b)] = (xp[two(b)].astype(F32) + u.astype(BF).astype(F32)).astype(BF)

    def pump(n, on):
        on(n - 1, lambda b: drain(0, b, th))
        on(n - 3, lambda b: drain(1, b, to))
        on(n - 5, lambda b: (drain(2, b, 2 * to), t_x(b).wait()))
        on(n - 7, lambda b: (drain(3, b, 2 * to), t_keep(b).wait()))
        on(n - 9, lambda b: drain(4, b, to))
        on(n - LAST, lambda b: drain(5, b, th))
        on(n - 3, sum_first)
        on(n - 5, sum_second)
        on(n - 1, sum_pair)
        on(n - 3, lambda b: (start(t_second(b)), t_x(b).start()))
        on(n - 5, lambda b: (start(t_own(b)), t_keep(b).start()))
        on(n - 1, lambda b: start(t_first(b)))
        on(n - 7, lambda b: start(t_pass(b)))
        on(n, lambda b: start(t_pair(b)))
        on(n - 9, lambda b: start(t_half(b)))

    def guarded(cond, b, g):
        @pl.when(cond)
        def _():
            g(b)

    def step(n):
        if COMM:
            @pl.when(n >= LAST)
            def _():
                pump(n, lambda b, g: g(b) and None)

            @pl.when(n < LAST)
            def _():
                pump(n, lambda b, g: guarded(b >= 0, b, g))

    def put_qkv(c, r, first):
        base = pl.multiple_of(lax.rem(c, per_seq) * tc, tc)
        for i in range(r.shape[1] // dh):
            head, kind = divmod(first // dh + i, 3)
            val = r[:, i * dh:(i + 1) * dh].astype(BF)
            if kind == 0:
                qb[head] = val
            else:
                (kc, vc)[kind - 1][head, pl.ds(base, tc), :] = val

    def attend(c):
        scale = dh ** -0.5 * math.log2(math.e)
        j = lax.rem(c, per_seq)
        qr = tc // 2
        block = min(64, qr)
        blocks = [slice(r, r + block) for r in range(0, qr, block)]

        def scores(h, i, tiles):
            width = (tiles - 1) * tc + (i + 1) * qr
            m = None
            for lo in range(0, width, tc):
                hi = min(lo + tc, width)
                st = lax.dot_general(qb[h, i * qr:(i + 1) * qr, :], kc[h, lo:hi, :], (((1,), (1,)), ((), ())), preferred_element_type=F32)
                if hi == width:
                    row = lax.broadcasted_iota(jnp.int32, st.shape, 0) + i * qr
                    st = jnp.where(row >= lax.broadcasted_iota(jnp.int32, st.shape, 1), st, -1e30)
                sb[i][:, lo:hi] = st
                for g in range(0, hi - lo, 128):
                    v = st[:, g:g + 128]
                    m = v if m is None else jnp.maximum(m, v)
            mt[i][...] = m

        def output(h, i, tiles):
            width = (tiles - 1) * tc + (i + 1) * qr
            sums = []
            for rb in blocks:
                top = jnp.max(mt[i][rb], axis=1, keepdims=True)
                e = jnp.exp2((sb[i][rb, 0:width] - top) * scale)
                sums.append(jnp.sum(e, axis=1, keepdims=True))
                e = e.astype(BF)
                for g in range(width // 128):
                    pb[i][rb.start // 16:rb.stop // 16, g] = e[:, g * 128:(g + 1) * 128].reshape(block // 16, 16, 128)
            p = jnp.concatenate([pb[i][:, g].reshape(qr, 128) for g in range(width // 128)], axis=1)
            o = jnp.dot(p, vc[h, 0:width, :], preferred_element_type=F32)
            for rb, total in zip(blocks, sums):
                first = (i * qr + rb.start) // 16
                hbuf[first:first + block // 16, f // 128 + h] = (o[rb] / total).astype(BF).reshape(block // 16, 16, 128)

        for tiles in range(1, per_seq + 1):
            @pl.when(j == tiles - 1)
            def _(tiles=tiles):
                scores(0, 0, tiles)

                def head(h, more):
                    scores(h, 1, tiles)
                    output(h, 0, tiles)
                    if more:
                        scores(h + 1, 0, tiles)
                    output(h, 1, tiles)

                if tiles <= UNROLL:
                    for h in range(hl):
                        head(h, h < hl - 1)
                else:
                    @pl.loop(0, (hl - 1) // 2)
                    def _(u):
                        head(2 * u, True)
                        head(2 * u + 1, True)
                    for h in range((hl - 1) // 2 * 2, hl):
                        head(h, h < hl - 1)

    def gelu(r):
        return 0.5 * r * (1.0 + lax.erf(r * (0.5 ** 0.5)))

    start(wload("q0", 0))
    xload(0, 0).start()
    if COMM:
        barrier = pltpu.get_barrier_semaphore()
        for dev in (partner, right, left):
            pl.semaphore_signal(barrier, inc=1, device_id=dev, device_id_type=pl.DeviceIdType.MESH)
        pl.semaphore_wait(barrier, 3)

    @pl.loop(0, 4)
    def _(i):
        @pl.when(i < 3)
        def _():
            xload(0, i + 1).start()
        xload(0, i).wait()
        norm(i)

    @pl.loop(0, chunks)
    def _(c):
        n0 = c * nk - 5
        nxt = jnp.minimum(c + 1, chunks - 1)

        step(n0)
        wait(wload("q0", 0))
        start(wload("q1", 1))
        put_qkv(c, jnp.dot(gather(ln), wbuf[0, 0:d, 0:qa], preferred_element_type=F32), 0)

        step(n0 + 1)
        wait(wload("q1", 1))
        start(wload("g", 0, 0))
        put_qkv(c, jnp.dot(gather(ln), wbuf[1, 0:d, 0:qw - qa], preferred_element_type=F32), qa)

        step(n0 + 2)
        attend(c)

        @pl.loop(0, 2)
        def _(i):
            step(n0 + 3 + i)
            wait(wload("g", i, i))

            @pl.when(i == 0)
            def _():
                start(wload("g", 1, 1))

            @pl.when(i == 1)
            def _():
                start(wload("d", 0, 0))
                xload(nxt, 0).start()

            r = jnp.dot(gather(ln), wbuf[i, 0:d, 0:gw], preferred_element_type=F32)
            scatter(hbuf, i * (gw // 128), gelu(r).astype(BF))

        @pl.loop(0, 4)
        def _(i):
            slot = lax.rem(i, 2)
            @pl.when(i > 0)
            def _():
                step(n0 + 4 + i)

            wait(wload("d", slot, i))
            xload(nxt, i).wait()

            @pl.when(i < 3)
            def _():
                start(wload("d", 1 - slot, i + 1))
                xload(nxt, i + 1).start()

            @pl.when(jnp.logical_and(i == 3, c < chunks - 1))
            def _():
                start(wload("q0", 0))

            b = c * nk + 2 * i
            cut = (dw // 2 + 255) // 256 * 256
            seen = norm(i)
            tiles = gather(hbuf)
            r0 = jnp.dot(tiles, wbuf[slot, 0:f + hd, 0:cut], preferred_element_type=F32)
            tiles = gather(hbuf, lambda v: jnp.where(me < 0, seen, v))
            r1 = jnp.dot(tiles, wbuf[slot, 0:f + hd, cut:dw], preferred_element_type=F32)
            part[ring(b)] = r0[:, 0:nb].astype(BF)
            part[ring(b + 1), :, 0:cut - nb] = r0[:, nb:cut].astype(BF)
            part[ring(b + 1), :, cut - nb:nb] = r1.astype(BF)

    if COMM:
        @pl.loop(nblk - 5, nblk + LAST)
        def _(n):
            pump(n, lambda b, g: guarded(b < nblk, b, g))


def layer(cfg, x, gamma, beta, wqkv, wo, w1, w2):
    (ntok, d, s, hl, dh, f, tc, tp) = cfg
    nb, to = d // 8, tc // tp
    any_ = pl.BlockSpec(memory_space=pl.ANY)
    vm = pl.BlockSpec(memory_space=pltpu.VMEM)
    qw = 3 * hl * dh
    qa = (qw // 2 + 255) // 256 * 256
    width = max(qa, qw - qa, f // 2, d // 4)
    depth = max(d, f + hl * dh)
    return pl.pallas_call(
        functools.partial(kernel, cfg),
        out_shape=jax.ShapeDtypeStruct((ntok, d), BF),
        in_specs=[any_, vm, vm, any_, any_, any_, any_],
        out_specs=any_,
        scratch_shapes=[
            pltpu.VMEM((2, depth, width), BF),
            pltpu.VMEM((tc // 16, d // 128, 16, 128), BF),
            pltpu.VMEM((hl, tc, dh), BF),
            pltpu.VMEM((hl, s, dh), BF),
            pltpu.VMEM((hl, s, dh), BF),
            pltpu.VMEM((tc // 16, (f + hl * dh) // 128, 16, 128), BF),
            pltpu.VMEM((RING, tc, nb), BF),
            pltpu.VMEM((2, tc // 4, d), BF),
            pltpu.VMEM((tc // 2, s - tc // 2), F32),
            pltpu.VMEM((tc // 2, s), F32),
            pltpu.VMEM((tc // 32, (s - tc // 2) // 128, 16, 128), BF),
            pltpu.VMEM((tc // 32, s // 128, 16, 128), BF),
            *[pltpu.VMEM((tc // 2, 128), F32) for _ in range(2)],
            pltpu.VMEM((2, tc // 2, nb), BF),
            pltpu.VMEM((DEPTH, to // 2, nb), BF),
            pltpu.VMEM((DEPTH, to // 2, nb), BF),
            pltpu.VMEM((DEPTH, to, nb), BF),
            pltpu.VMEM((DEPTH, to, nb), BF),
            pltpu.VMEM((2, to, nb), BF),
            pltpu.VMEM((2, to, nb), BF),
            pltpu.SemaphoreType.DMA((2, 2)),
            pltpu.SemaphoreType.DMA((2,)),
            pltpu.SemaphoreType.DMA((CHANNELS, DEPTH)),
            pltpu.SemaphoreType.DMA((CHANNELS, DEPTH)),
            pltpu.SemaphoreType.DMA((DEPTH,)),
            pltpu.SemaphoreType.DMA((DEPTH,)),
        ],
        compiler_params=pltpu.CompilerParams(
            collective_id=0 if COMM else None, has_side_effects=True, vmem_limit_bytes=67043328),
        name="layer",
    )(x, gamma, beta, wqkv, wo, w1, w2)


def solution(mesh):
    tp = mesh.shape["tp"]

    def local(x, gamma, beta, wqkv, wo, w1, w2):
        b, s, d = x.shape
        hl, dh, _ = wo.shape
        cfg = (b * s, d, s, hl, dh, w1.shape[1], s // 4, tp)
        y = layer(cfg, x.reshape(b * s, d), gamma.reshape(1, d), beta.reshape(1, d),
                  wqkv, wo.reshape(hl * dh, d), w1, w2)
        return y.reshape(b, s, d)

    return jax.shard_map(local, mesh=mesh,
                         in_specs=(P('dp', None, None), P(None), P(None), P(None, 'tp'),
                                   P('tp', None, None), P(None, 'tp'), P('tp', None)),
                         out_specs=P('dp', None, None), check_vma=False)
```

```python
import functools
import math

import jax
import jax.numpy as jnp
from jax import lax
from jax.experimental import pallas as pl
from jax.experimental.pallas import tpu as pltpu
from jax.sharding import PartitionSpec as P

BF = jnp.bfloat16
F32 = jnp.float32
DEPTH = 4
RING = 10
LAST = 11
CHANNELS = 6
COMM = True
UNROLL = 2


def kernel(cfg, x, gamma, beta, wqkv, wo, w1, w2, y,
           wbuf, ln, qb, kc, vc, hbuf, part, xbuf, sb0, sb1, pb0, pb1, mt0, mt1, s1r, r1l, r1r, r2l, r2r, ybuf, xp,
           wsem, xsem, ssem, rsem, ysem, xpsem):
    (ntok, d, s, hl, dh, f, tc, tp) = cfg
    sb, pb, mt = (sb0, sb1), (pb0, pb1), (mt0, mt1)
    hd = hl * dh
    chunks, per_seq = ntok // tc, s // tc
    nk = 8
    nb, dw, gw = d // nk, d // 4, f // 2
    qw = 3 * hd
    qa = (qw // 2 + 255) // 256 * 256
    th, to = tc // 2, tc // tp
    half = to // 2
    lnr = tc // 4
    nblk = chunks * nk
    nx = tp // 2

    me = lax.axis_index("tp")
    cx, q = me // 2, me % 2
    right = {"tp": ((cx + 1) % nx) * 2 + q}
    left = {"tp": ((cx + nx - 1) % nx) * 2 + q}
    partner = {"tp": cx * 2 + 1 - q}
    o_me = q * th + cx * to
    o_right = q * th + ((cx + 1) % nx) * to
    o_left = q * th + ((cx + nx - 1) % nx) * to
    o_opp = q * th + ((cx + 2) % nx) * to
    mine, theirs = q * th, (1 - q) * th

    def rows(start, size):
        return pl.ds(pl.multiple_of(start, math.gcd(size, half)), size)

    def wload(step, slot, i=None):
        if step == "q0":
            return [pltpu.make_async_copy(wqkv.at[:, 0:qa], wbuf.at[slot, 0:d, 0:qa], wsem.at[slot, 0])]
        if step == "q1":
            return [pltpu.make_async_copy(wqkv.at[:, qa:qw], wbuf.at[slot, 0:d, 0:qw - qa], wsem.at[slot, 0])]
        if step == "g":
            return [pltpu.make_async_copy(w1.at[:, pl.ds(pl.multiple_of(i * gw, 128), gw)], wbuf.at[slot, 0:d, 0:gw], wsem.at[slot, 0])]
        cols = pl.ds(pl.multiple_of(i * dw, 128), dw)
        return [pltpu.make_async_copy(w2.at[:, cols], wbuf.at[slot, 0:f, 0:dw], wsem.at[slot, 0]),
                pltpu.make_async_copy(wo.at[:, cols], wbuf.at[slot, f:f + hd, 0:dw], wsem.at[slot, 1])]

    def start(copies):
        for copy in copies:
            copy.start()

    def wait(copies):
        for copy in copies:
            copy.wait()

    def gather(tiles, corner=None):
        parts = [tiles[:, g].reshape(tc, 128) for g in range(tiles.shape[1])]
        if corner:
            parts[0] = jnp.concatenate([corner(parts[0][:8]), parts[0][8:]], axis=0)
        return jnp.concatenate(parts, axis=1)

    def scatter(tiles, first, val):
        for g in range(val.shape[1] // 128):
            tiles[:, first + g] = val[:, g * 128:(g + 1) * 128].reshape(tc // 16, 16, 128)

    def xload(c, i):
        return pltpu.make_async_copy(x.at[pl.ds(pl.multiple_of(c * tc + i * lnr, lnr), lnr), :], xbuf.at[i % 2], xsem.at[i % 2])

    def norm(i):
        sub = 8
        seen = None
        for r in range(lnr // sub):
            xs = xbuf[i % 2, r * sub:(r + 1) * sub, :].astype(F32)
            xc = xs - jnp.sum(xs, axis=-1, keepdims=True) * (1.0 / d)
            inv = lax.rsqrt(jnp.sum(xc * xc, axis=-1, keepdims=True) * (1.0 / d) + 1e-5)
            out = (xc * inv * gamma[...] + beta[...]).astype(BF)
            for g in range(d // 128):
                v = out[:, g * 128:(g + 1) * 128]
                ln[i * (lnr // 16) + r // 2, g, r % 2 * 8:r % 2 * 8 + 8] = v
                seen = v if seen is None else jnp.maximum(seen, v)
        return seen

    def k(b):
        return lax.rem(b + 16, DEPTH)

    def two(b):
        return lax.rem(b + 16, 2)

    def ring(b):
        return lax.rem(b + 2 * RING, RING)

    def y_at(b, off, size):
        c, kk = b // nk, b % nk
        return y.at[rows(c * tc + off, size), pl.ds(pl.multiple_of(kk * nb, 128), nb)]

    def remote(ch, b, src, dst, dev):
        return pltpu.make_async_remote_copy(src, dst, ssem.at[ch, k(b)], rsem.at[ch, k(b)], device_id=dev, device_id_type=pl.DeviceIdType.MESH)

    def t_pair(b):
        return remote(0, b, part.at[ring(b), rows(theirs, th), :], s1r.at[two(b)], partner)

    def t_first(b, side):
        p = ring(b)
        if side == 0:
            return remote(1, b, part.at[p, rows(o_opp, half), :], r1l.at[k(b)], right)
        return remote(1, b, part.at[p, rows(o_opp + half, half), :], r1r.at[k(b)], left)

    def t_second(b, side):
        p = ring(b)
        if side == 0:
            return remote(2, b, part.at[p, rows(o_right, to), :], r2l.at[k(b)], right)
        return remote(2, b, part.at[p, rows(o_left, to), :], r2r.at[k(b)], left)

    def t_own(b, side):
        return remote(3, b, ybuf.at[two(b)], y_at(b, o_me, to), (right, left)[side])

    def t_keep(b):
        return pltpu.make_async_copy(ybuf.at[two(b)], y_at(b, o_me, to), ysem.at[k(b)])

    def t_pass(b, side):
        at = y_at(b, o_right + half if side else o_left, half)
        return remote(4, b, at, at, (right, left)[side])

    def t_half(b):
        at = y_at(b, mine, th)
        return remote(5, b, at, at, partner)

    def t_x(b):
        c, kk = b // nk, b % nk
        return pltpu.make_async_copy(x.at[rows(c * tc + o_me, to), pl.ds(pl.multiple_of(kk * nb, 128), nb)], xp.at[two(b)], xpsem.at[k(b)])

    def drain(ch, b, size):
        ref = part.at[0, 0:size, :]
        copy = remote(ch, b, ref, ref, partner)
        copy.wait_recv()
        copy.wait_send()

    def sum_pair(b):
        p, at = ring(b), rows(mine, th)
        part[p, at, :] = part[p, at, :] + s1r[two(b)]

    def sum_first(b):
        p = ring(b)
        at = rows(o_right, half)
        part[p, at, :] = part[p, at, :] + r1l[k(b)]
        at = rows(o_left + half, half)
        part[p, at, :] = part[p, at, :] + r1r[k(b)]

    def sum_second(b):
        u = part[ring(b), rows(o_me, to), :].astype(F32) + (r2l[k(b)].astype(F32) + r2r[k(b)].astype(F32))
        ybuf[two(b)] = (xp[two(b)].astype(F32) + u.astype(BF).astype(F32)).astype(BF)

    def pump(n, on):
        on(n - 1, lambda b: drain(0, b, th))
        on(n - 3, lambda b: drain(1, b, to))
        on(n - 5, lambda b: (drain(2, b, 2 * to), t_x(b).wait()))
        on(n - 7, lambda b: (drain(3, b, 2 * to), t_keep(b).wait()))
        on(n - 9, lambda b: drain(4, b, to))
        on(n - LAST, lambda b: drain(5, b, th))
        on(n - 3, sum_first)
        on(n - 5, sum_second)
        on(n - 1, sum_pair)
        for side in range(2):
            on(n - 1, lambda b: t_first(b, side).start())
            on(n - 3, lambda b: t_second(b, side).start())
            on(n - 7, lambda b: t_pass(b, side).start())
            on(n - 5, lambda b: t_own(b, side).start())
        on(n, lambda b: t_pair(b).start())
        on(n - 9, lambda b: t_half(b).start())
        on(n - 3, lambda b: t_x(b).start())
        on(n - 5, lambda b: t_keep(b).start())

    def guarded(cond, b, g):
        @pl.when(cond)
        def _():
            g(b)

    def step(n):
        if COMM:
            @pl.when(n >= LAST)
            def _():
                pump(n, lambda b, g: g(b) and None)

            @pl.when(n < LAST)
            def _():
                pump(n, lambda b, g: guarded(b >= 0, b, g))

    def put_qkv(c, r, first):
        base = pl.multiple_of(lax.rem(c, per_seq) * tc, tc)
        for i in range(r.shape[1] // dh):
            head, kind = divmod(first // dh + i, 3)
            val = r[:, i * dh:(i + 1) * dh].astype(BF)
            if kind == 0:
                qb[head] = val
            else:
                (kc, vc)[kind - 1][head, pl.ds(base, tc), :] = val

    def attend(c):
        scale = dh ** -0.5 * math.log2(math.e)
        j = lax.rem(c, per_seq)
        qr = tc // 2
        block = min(64, qr)
        blocks = [slice(r, r + block) for r in range(0, qr, block)]

        def scores(h, i, tiles):
            width = (tiles - 1) * tc + (i + 1) * qr
            m = None
            for lo in range(0, width, tc):
                hi = min(lo + tc, width)
                st = lax.dot_general(qb[h, i * qr:(i + 1) * qr, :], kc[h, lo:hi, :], (((1,), (1,)), ((), ())), preferred_element_type=F32)
                if hi == width:
                    row = lax.broadcasted_iota(jnp.int32, st.shape, 0) + i * qr
                    st = jnp.where(row >= lax.broadcasted_iota(jnp.int32, st.shape, 1), st, -1e30)
                sb[i][:, lo:hi] = st
                for g in range(0, hi - lo, 128):
                    v = st[:, g:g + 128]
                    m = v if m is None else jnp.maximum(m, v)
            mt[i][...] = m

        def output(h, i, tiles):
            width = (tiles - 1) * tc + (i + 1) * qr
            sums = []
            for rb in blocks:
                top = jnp.max(mt[i][rb], axis=1, keepdims=True)
                e = jnp.exp2((sb[i][rb, 0:width] - top) * scale)
                sums.append(jnp.sum(e, axis=1, keepdims=True))
                e = e.astype(BF)
                for g in range(width // 128):
                    pb[i][rb.start // 16:rb.stop // 16, g] = e[:, g * 128:(g + 1) * 128].reshape(block // 16, 16, 128)
            p = jnp.concatenate([pb[i][:, g].reshape(qr, 128) for g in range(width // 128)], axis=1)
            o = jnp.dot(p, vc[h, 0:width, :], preferred_element_type=F32)
            for rb, total in zip(blocks, sums):
                first = (i * qr + rb.start) // 16
                hbuf[first:first + block // 16, f // 128 + h] = (o[rb] / total).astype(BF).reshape(block // 16, 16, 128)

        for tiles in range(1, per_seq + 1):
            @pl.when(j == tiles - 1)
            def _(tiles=tiles):
                scores(0, 0, tiles)

                def head(h, more):
                    scores(h, 1, tiles)
                    output(h, 0, tiles)
                    if more:
                        scores(h + 1, 0, tiles)
                    output(h, 1, tiles)

                if tiles <= UNROLL:
                    for h in range(hl):
                        head(h, h < hl - 1)
                else:
                    @pl.loop(0, (hl - 1) // 2)
                    def _(u):
                        head(2 * u, True)
                        head(2 * u + 1, True)
                    for h in range((hl - 1) // 2 * 2, hl):
                        head(h, h < hl - 1)

    def gelu(r):
        return 0.5 * r * (1.0 + lax.erf(r * (0.5 ** 0.5)))

    start(wload("q0", 0))
    xload(0, 0).start()
    if COMM:
        barrier = pltpu.get_barrier_semaphore()
        for dev in (partner, right, left):
            pl.semaphore_signal(barrier, inc=1, device_id=dev, device_id_type=pl.DeviceIdType.MESH)

    @pl.loop(0, 4)
    def _(i):
        @pl.when(i < 3)
        def _():
            xload(0, i + 1).start()
        xload(0, i).wait()
        norm(i)

    if COMM:
        pl.semaphore_wait(barrier, 3)

    @pl.loop(0, chunks)
    def _(c):
        n0 = c * nk - 5
        nxt = jnp.minimum(c + 1, chunks - 1)

        step(n0)
        wait(wload("q0", 0))
        start(wload("q1", 1))
        put_qkv(c, jnp.dot(gather(ln), wbuf[0, 0:d, 0:qa], preferred_element_type=F32), 0)

        step(n0 + 1)
        wait(wload("q1", 1))
        start(wload("g", 0, 0))
        put_qkv(c, jnp.dot(gather(ln), wbuf[1, 0:d, 0:qw - qa], preferred_element_type=F32), qa)

        step(n0 + 2)
        attend(c)

        @pl.loop(0, 2)
        def _(i):
            step(n0 + 3 + i)
            wait(wload("g", i, i))

            @pl.when(i == 0)
            def _():
                start(wload("g", 1, 1))

            @pl.when(i == 1)
            def _():
                start(wload("d", 0, 0))
                xload(nxt, 0).start()

            r = jnp.dot(gather(ln), wbuf[i, 0:d, 0:gw], preferred_element_type=F32)
            scatter(hbuf, i * (gw // 128), gelu(r).astype(BF))

        @pl.loop(0, 4)
        def _(i):
            slot = lax.rem(i, 2)
            @pl.when(i > 0)
            def _():
                step(n0 + 4 + i)

            wait(wload("d", slot, i))
            xload(nxt, i).wait()

            @pl.when(i < 3)
            def _():
                start(wload("d", 1 - slot, i + 1))
                xload(nxt, i + 1).start()

            @pl.when(jnp.logical_and(i == 3, c < chunks - 1))
            def _():
                start(wload("q0", 0))

            b = c * nk + 2 * i
            cut = min((dw // 2 + 255) // 256 * 256, dw - 128)
            seen = norm(i)
            tiles = gather(hbuf)
            r0 = jnp.dot(tiles, wbuf[slot, 0:f + hd, 0:cut], preferred_element_type=F32)
            tiles = gather(hbuf, lambda v: jnp.where(me < 0, seen, v))
            r1 = jnp.dot(tiles, wbuf[slot, 0:f + hd, cut:dw], preferred_element_type=F32)
            part[ring(b)] = r0[:, 0:nb].astype(BF)
            part[ring(b + 1), :, 0:cut - nb] = r0[:, nb:cut].astype(BF)
            part[ring(b + 1), :, cut - nb:nb] = r1.astype(BF)

    if COMM:
        @pl.loop(nblk - 5, nblk + LAST)
        def _(n):
            pump(n, lambda b, g: guarded(b < nblk, b, g))


def layer(cfg, x, gamma, beta, wqkv, wo, w1, w2):
    (ntok, d, s, hl, dh, f, tc, tp) = cfg
    nb, to = d // 8, tc // tp
    any_ = pl.BlockSpec(memory_space=pl.ANY)
    vm = pl.BlockSpec(memory_space=pltpu.VMEM)
    qw = 3 * hl * dh
    qa = (qw // 2 + 255) // 256 * 256
    width = max(qa, qw - qa, f // 2, d // 4)
    depth = max(d, f + hl * dh)
    return pl.pallas_call(
        functools.partial(kernel, cfg),
        out_shape=jax.ShapeDtypeStruct((ntok, d), BF),
        in_specs=[any_, vm, vm, any_, any_, any_, any_],
        out_specs=any_,
        scratch_shapes=[
            pltpu.VMEM((2, depth, width), BF),
            pltpu.VMEM((tc // 16, d // 128, 16, 128), BF),
            pltpu.VMEM((hl, tc, dh), BF),
            pltpu.VMEM((hl, s, dh), BF),
            pltpu.VMEM((hl, s, dh), BF),
            pltpu.VMEM((tc // 16, (f + hl * dh) // 128, 16, 128), BF),
            pltpu.VMEM((RING, tc, nb), BF),
            pltpu.VMEM((2, tc // 4, d), BF),
            pltpu.VMEM((tc // 2, s - tc // 2), F32),
            pltpu.VMEM((tc // 2, s), F32),
            pltpu.VMEM((tc // 32, (s - tc // 2) // 128, 16, 128), BF),
            pltpu.VMEM((tc // 32, s // 128, 16, 128), BF),
            *[pltpu.VMEM((tc // 2, 128), F32) for _ in range(2)],
            pltpu.VMEM((2, tc // 2, nb), BF),
            pltpu.VMEM((DEPTH, to // 2, nb), BF),
            pltpu.VMEM((DEPTH, to // 2, nb), BF),
            pltpu.VMEM((DEPTH, to, nb), BF),
            pltpu.VMEM((DEPTH, to, nb), BF),
            pltpu.VMEM((2, to, nb), BF),
            pltpu.VMEM((2, to, nb), BF),
            pltpu.SemaphoreType.DMA((2, 2)),
            pltpu.SemaphoreType.DMA((2,)),
            pltpu.SemaphoreType.DMA((CHANNELS, DEPTH)),
            pltpu.SemaphoreType.DMA((CHANNELS, DEPTH)),
            pltpu.SemaphoreType.DMA((DEPTH,)),
            pltpu.SemaphoreType.DMA((DEPTH,)),
        ],
        compiler_params=pltpu.CompilerParams(
            collective_id=0 if COMM else None, has_side_effects=True, vmem_limit_bytes=67043328),
        name="layer",
    )(x, gamma, beta, wqkv, wo, w1, w2)


def move(y, block):
    def kernel_(a, b):
        b[...] = a[...]

    spec = pl.BlockSpec((block, y.shape[1]), lambda i: (i, 0))
    return pl.pallas_call(
        kernel_, grid=(y.shape[0] // block,), out_shape=jax.ShapeDtypeStruct(y.shape, y.dtype),
        in_specs=[spec], out_specs=spec, name="move",
        compiler_params=pltpu.CompilerParams(vmem_limit_bytes=40 * 2 ** 20))(y)


def solution(mesh):
    tp = mesh.shape["tp"]

    def local(x, gamma, beta, wqkv, wo, w1, w2):
        b, s, d = x.shape
        hl, dh, _ = wo.shape
        cfg = (b * s, d, s, hl, dh, w1.shape[1], s // 4, tp)
        y = layer(cfg, x.reshape(b * s, d), gamma.reshape(1, d), beta.reshape(1, d),
                  wqkv, wo.reshape(hl * dh, d), w1, w2)
        return move(y, cfg[6]).reshape(b, s, d)

    return jax.shard_map(local, mesh=mesh,
                         in_specs=(P('dp', None, None), P(None), P(None), P(None, 'tp'),
                                   P('tp', None, None), P(None, 'tp'), P('tp', None)),
                         out_specs=P('dp', None, None), check_vma=False)
```
